32 devices in a mesh: ctx: 16 (over z, y, x), work: 2 (over core).
Axes of the slice: x: 2, y: 2, z: 4, core: 2. Of those that a mesh axis runs over, the one named last changes fastest.
Arguments:
- inputs: bfloat16 [2, 4096, 2880], P('work', 'ctx'), may hold values from -6 to 6
- queries: bfloat16 [2, 4096, 2048], P('work', 'ctx')
- keys: bfloat16 [2, 4096, 256], P('work', 'ctx')
- out_grad: bfloat16 [2, 4096, 2048], P('work', 'ctx'), may hold values from -6 to 6
- positions: int32 [2, 4096], P('work', 'ctx'), may hold values from 0 to 4095, as said below
- bands: int32 [32], replicated, may hold values from 32 to 128, as said below
- step: int32 [1], replicated, may hold values from 1 to 16
- value_weight: float32 [2, 2880, 256], P('work', 'ctx'), may hold values from -0.109375 to 0.109375
- moment_one: float32 [2, 2880, 256], P('work', 'ctx'), may hold values from -0.0078125 to 0.0078125
- moment_two: float32 [2, 2880, 256], P('work', 'ctx'), may hold values from 1e-08 to 1e-06
Outputs:
- attn_out: bfloat16 [2, 4096, 2048], P('work', 'ctx')
- mean_weight: float32 [2880, 256], P('ctx')
- mean_one: float32 [2880, 256], P('ctx')
- mean_two: float32 [2880, 256], P('ctx')
The draws below stay inside these ranges and needn't reach their ends.
Inputs may be any that keep to these rules, and one draw needn't show every extreme that they name: `positions`: in each worker's sequence a token's position is 0 at the first token and at each document start, else one more than the previous token's. One worker's sequence is a single document. `bands`: one head has exactly 128.
All inputs are finite; a program needn't handle non-finite values.
Results may differ from the reference program's by a relative error of at most 0.0015.
The reference program's roundings to bfloat16 on the way count: a program that leaves them out, or rounds other values in their place, can miss the bound.
Values may be sent and summed in bfloat16 or wider, within the bound.
No kernel may reach another device: no remote copies, remote signals or barrier semaphores. Data moves between devices by JAX's collectives and lax.ppermute only.
A program may use at most 64 MiB of HBM per device.

```python
import math
import jax
import jax.numpy as jnp
from jax import lax

D = 2880
HD = 64
QH = 32
KH = 4
LOOKBACK_SPAN = 128
TOKENS_PER_UNIT = 256
TOKENS = 4096
WORKERS = 2
N_CTX = 16
N_WORK = 2


def shared_keys(key):
    return jax.random.normal(jax.random.fold_in(key, 7), (WORKERS, TOKENS, KH * HD), jnp.float32)


def draw_keys(key, part):
    return shared_keys(key).astype(jnp.bfloat16)


def draw_queries(key, part):
    base = jax.random.normal(jax.random.fold_in(key, 13), (WORKERS, TOKENS, QH * HD), jnp.float32)
    return base.astype(jnp.bfloat16)


def draw_positions(key, part):
    index = jnp.broadcast_to(jnp.arange(TOKENS, dtype=jnp.int32), (WORKERS, TOKENS))
    worker = jnp.broadcast_to(jnp.arange(WORKERS, dtype=jnp.int32)[:, None], (WORKERS, TOKENS))
    single = jax.random.randint(jax.random.fold_in(key, 37), (), 0, WORKERS)
    starts = jax.random.randint(jax.random.fold_in(key, 23), (WORKERS, TOKENS), 0, 2 * TOKENS_PER_UNIT) == 0
    starts = starts & (worker != single) | (index == 0)
    begun = jax.lax.cummax(jnp.where(starts, index, 0), axis=1)
    return (index - begun).astype(jnp.int32)


def draw_bands(key, part):
    widths = jax.random.randint(jax.random.fold_in(key, 29), (QH,), LOOKBACK_SPAN // 4, LOOKBACK_SPAN + 1)
    chosen = jax.random.randint(jax.random.fold_in(key, 31), (1,), 0, QH)
    return jnp.where(jnp.arange(QH, dtype=jnp.int32) == chosen, LOOKBACK_SPAN, widths).astype(jnp.int32)


def levels(rng, extent, cuts, least, top_value):
    factor_of = 1.0
    for position, blocks in cuts:
        draws = jax.random.uniform(jax.random.fold_in(jax.random.fold_in(rng, 6), position), (blocks,), jnp.float32, least / len(cuts), top_value / len(cuts))
        factor_of = factor_of * jnp.repeat(jnp.exp(draws), extent[position] // blocks).reshape((-1,) + (1,) * (len(extent) - 1 - position))
    return factor_of


def gaussian(key, extent, spread, reach, shards=(), held_as=jnp.bfloat16):
    loudness = levels(key, extent, shards, -0.22, 0.18) if shards else 1.0
    entries = jax.random.normal(key, extent, jnp.float32) * spread * loudness
    return jnp.minimum(jnp.maximum(entries, -reach), reach).astype(held_as)


def setup_inputs(seed: int = 0) -> dict:
    arg_keys = jax.random.split(jax.random.key(seed), 11)
    inputs = gaussian(arg_keys[0], (WORKERS, TOKENS, D), 1.0, 6.0, ((0, 2), (1, 16)))
    queries = draw_queries(jax.random.fold_in(arg_keys[10], 71), 0)
    keys = draw_keys(jax.random.fold_in(arg_keys[10], 71), 0)
    out_grad = gaussian(arg_keys[3], (WORKERS, TOKENS, QH * HD), 1.0, 6.0, ((0, 2), (1, 16)))
    positions = draw_positions(jax.random.fold_in(arg_keys[10], 71), 0)
    bands = draw_bands(jax.random.fold_in(arg_keys[10], 71), 0)
    step = jax.random.randint(arg_keys[6], (1,), 1, 17).astype(jnp.int32)
    value_weight = gaussian(arg_keys[7], (WORKERS, D, KH * HD), D ** -0.5, 0.109375, ((0, 2), (1, 16)), jnp.float32)
    moment_one = gaussian(arg_keys[8], (WORKERS, D, KH * HD), 0.0005, 0.0078125, ((0, 2), (1, 16)), jnp.float32)
    moment_two = jnp.clip(jnp.exp(math.log(9.999999974752427e-07) - 4.6051702 * jax.random.uniform(arg_keys[9], (WORKERS, D, KH * HD), jnp.float32) ** levels(arg_keys[9], (WORKERS, D, KH * HD), ((0, 2), (1, 16)), -0.2, 0.2)), 9.99999993922529e-09, 9.999999974752427e-07)
    return dict(inputs=inputs, queries=queries, keys=keys, out_grad=out_grad, positions=positions, bands=bands, step=step, value_weight=value_weight, moment_one=moment_one, moment_two=moment_two)


beta_one = 0.9
beta_two = 0.95
adam_eps = 1e-08
learn_rate = 0.01
clip_norm = 0.5

def attend(qrows, krows, vrows, grows, bands, pos):
    count = qrows.shape[0]
    span = krows.shape[0]
    halo = span - count
    group = QH // KH
    dist = lax.broadcasted_iota(jnp.int32, (count, span), 0) + halo - lax.broadcasted_iota(jnp.int32, (count, span), 1)
    near = (dist >= 0) & (dist <= pos[:, None])
    outputs = []
    grads = []
    for head in range(KH):
        lo = head * group * HD
        hi = (head + 1) * group * HD
        query = qrows[:, lo:hi].reshape(count, group, HD).astype(jnp.float32)
        keyed = krows[:, head * HD:(head + 1) * HD].astype(jnp.float32)
        valued = vrows[:, head * HD:(head + 1) * HD].astype(jnp.float32)
        cotan = grows[:, lo:hi].reshape(count, group, HD).astype(jnp.float32)
        limit = bands[head * group:(head + 1) * group]
        allowed = near[None] & (dist[None] <= limit[:, None, None])
        scores = jnp.einsum('qgd,kd->gqk', query, keyed) * HD ** (-0.5)
        scores = jnp.where(allowed, scores, -1e+30)
        top = lax.optimization_barrier(jnp.max(scores, axis=2, keepdims=True))
        expo = jnp.exp(scores - top)
        probs = (expo / lax.optimization_barrier(jnp.sum(expo, axis=2, keepdims=True))).astype(jnp.bfloat16).astype(jnp.float32)
        outputs.append(jnp.einsum('gqk,kd->qgd', probs, valued).reshape(count, group * HD))
        grads.append(jnp.einsum('gqk,qgd->kd', probs, cotan))
    return (jnp.concatenate(outputs, 1).astype(jnp.bfloat16), jnp.concatenate(grads, 1))

def reference(inputs, queries, keys, out_grad, positions, bands, step, value_weight, moment_one, moment_two):
    window_extent = KH * HD

    def one_worker(items):
        acts, query, keyed, cotan, pos, weight, first, second = items
        value_vectors = jnp.dot(acts, weight.astype(jnp.bfloat16), preferred_element_type=jnp.float32).astype(jnp.bfloat16)
        kpad = jnp.concatenate([jnp.zeros((LOOKBACK_SPAN, window_extent), jnp.bfloat16), keyed], 0)
        value_padded = jnp.concatenate([jnp.zeros((LOOKBACK_SPAN, window_extent), jnp.bfloat16), value_vectors], 0)

        def block(dv_pad, index):
            begin_offset = (index * TOKENS_PER_UNIT).astype(jnp.int32)
            qb = lax.dynamic_slice_in_dim(query, begin_offset, TOKENS_PER_UNIT, 0)
            gb = lax.dynamic_slice_in_dim(cotan, begin_offset, TOKENS_PER_UNIT, 0)
            pb = lax.dynamic_slice_in_dim(pos, begin_offset, TOKENS_PER_UNIT, 0)
            kb = lax.dynamic_slice_in_dim(kpad, begin_offset, TOKENS_PER_UNIT + LOOKBACK_SPAN, 0)
            value_band_rows = lax.dynamic_slice_in_dim(value_padded, begin_offset, TOKENS_PER_UNIT + LOOKBACK_SPAN, 0)
            out, grad_block = attend(qb, kb, value_band_rows, gb, bands, pb)
            current = lax.dynamic_slice_in_dim(dv_pad, begin_offset, TOKENS_PER_UNIT + LOOKBACK_SPAN, 0)
            dv_pad = lax.dynamic_update_slice_in_dim(dv_pad, current + grad_block, begin_offset, 0)
            return (dv_pad, out)
        dv_pad, outs = lax.scan(block, jnp.zeros((TOKENS + LOOKBACK_SPAN, window_extent), jnp.float32), jnp.arange(N_CTX, dtype=jnp.int32))
        value_grad = dv_pad[LOOKBACK_SPAN:].astype(jnp.bfloat16)
        grad = jnp.dot(acts.T, value_grad, preferred_element_type=jnp.float32) / TOKENS
        norm = jnp.sqrt(jnp.sum(grad * grad))
        grad = grad * jnp.minimum(1.0, clip_norm / (norm + 1e-06))
        first = beta_one * first + (1.0 - beta_one) * grad
        second = beta_two * second + (1.0 - beta_two) * grad * grad
        count = step[0].astype(jnp.float32)
        fix_one = 1.0 - jnp.power(jnp.float32(beta_one), count)
        fix_two = 1.0 - jnp.power(jnp.float32(beta_two), count)
        weight = weight - learn_rate * (first / fix_one) / (jnp.sqrt(second / fix_two) + adam_eps)
        return (outs.reshape(TOKENS, QH * HD), weight, first, second)
    outs, weights, firsts, seconds = lax.map(one_worker, (inputs, queries, keys, out_grad, positions, value_weight, moment_one, moment_two))
    return (outs, lax.optimization_barrier(jnp.sum(weights, axis=0)) / N_WORK, lax.optimization_barrier(jnp.sum(firsts, axis=0)) / N_WORK, lax.optimization_barrier(jnp.sum(seconds, axis=0)) / N_WORK)
```

```python
import functools

import jax
import jax.numpy as jnp
from jax import lax
from jax.experimental import pallas as pl
from jax.experimental.pallas import tpu as pltpu
from jax.sharding import PartitionSpec as P


HD = 64
QH = 32
KH = 4
LOOKBACK_SPAN = 128
LANES = 128

beta_one = 0.9
beta_two = 0.95
adam_eps = 1e-08
learn_rate = 0.01
clip_norm = 0.5

bf16 = jnp.bfloat16
f32 = jnp.float32


def swapped(array, axis, mask):
    pairs = [(i, i ^ mask) for i in range(lax.axis_size(axis))]
    return lax.ppermute(array, axis, pairs)


def shifted(array, axis, by):
    devices = lax.axis_size(axis)
    pairs = [(i, i + by) for i in range(devices) if 0 <= i + by < devices]
    return lax.ppermute(array, axis, pairs)


VMEM = pl.BlockSpec(memory_space=pltpu.VMEM)
SMEM = pl.BlockSpec(memory_space=pltpu.SMEM)


def params(mib):
    return pltpu.CompilerParams(vmem_limit_bytes=mib << 20)


def full(shape, dtype):
    return jax.ShapeDtypeStruct(shape, dtype)


def probs_body(bands, pos, query, cotan, klo, khi, probs_out, grad_out):
    block = LOOKBACK_SPAN
    group = QH // KH
    pairs = group // 2
    step = pl.program_id(0)
    span = 2 * block
    left = lax.broadcasted_iota(jnp.int32, (span, LANES), 1) < HD
    keyed = jnp.concatenate([klo[...], khi[...]], 0).astype(f32) * HD ** (-0.5)
    rolled = pltpu.roll(keyed, HD, 1)
    dist = (
        lax.broadcasted_iota(jnp.int32, (span, block), 1)
        + block
        - lax.broadcasted_iota(jnp.int32, (span, block), 0)
    )
    dist = jnp.where(dist < 0, 2 * span, dist)
    row = pos[...]
    sums = []
    for half in range(2):
        one, two = (keyed, rolled) if half == 0 else (rolled, keyed)
        sides = (
            jnp.where(left, one, 0.0).astype(bf16),
            jnp.where(left, 0.0, two).astype(bf16),
        )
        base = half * group * HD
        cols = [slice(base + p * LANES, base + (p + 1) * LANES) for p in range(pairs)]
        queries = jnp.concatenate([query[:, c] for c in cols], 0)
        cotans = jnp.concatenate([cotan[:, c] for c in cols], 0)
        for odd, side in enumerate(sides):
            scores = lax.dot_general(
                side, queries, (((1,), (1,)), ((), ())), preferred_element_type=f32
            )
            rows = []
            for p in range(pairs):
                head = half * group + 2 * p + odd
                limit = jnp.minimum(row, bands[step * 2 * group + head])
                seen = jnp.where(
                    dist <= limit, scores[:, p * block : (p + 1) * block], -1e30
                )
                expo = jnp.exp(seen - jnp.max(seen, axis=0, keepdims=True))
                prob = (expo * (1.0 / jnp.sum(expo, axis=0, keepdims=True))).astype(bf16)
                probs_out[head] = prob
                rows.append(prob)
            sums.append(
                lax.dot_general(
                    jnp.concatenate(rows, 1),
                    cotans,
                    (((1,), (0,)), ((), ())),
                    preferred_element_type=f32,
                )
            )
    grad_out[...] = jnp.where(
        left,
        sums[0] + pltpu.roll(sums[1], HD, 1),
        sums[3] + pltpu.roll(sums[2], HD, 1),
    )


def probs_call(bands, positions, queries, out_grad, keys_lo, lo, keys_hi, hi, block_index):
    block = LOOKBACK_SPAN
    wide = 2 * (QH // KH) * HD
    heads = 2 * (QH // KH)
    steps = KH // 2
    return pl.pallas_call(
        probs_body,
        grid=(steps,),
        in_specs=[
            pl.BlockSpec(memory_space=pltpu.SMEM),
            pl.BlockSpec((1, block), lambda s: (0, block_index)),
            pl.BlockSpec((block, wide), lambda s: (block_index, s)),
            pl.BlockSpec((block, wide), lambda s: (block_index, s)),
            pl.BlockSpec((block, LANES), lambda s: (lo, s)),
            pl.BlockSpec((block, LANES), lambda s: (hi, s)),
        ],
        out_specs=[
            pl.BlockSpec((heads, 2 * block, block), lambda s: (s, 0, 0)),
            pl.BlockSpec((2 * block, LANES), lambda s: (0, s)),
        ],
        out_shape=[
            full((QH, 2 * block, block), bf16),
            full((2 * block, KH * HD), f32),
        ],
        compiler_params=params(16),
    )(bands, positions, queries, out_grad, keys_lo, keys_hi)


def mix_body(probs, vlo, vhi, *refs):
    out = refs[-1]
    group = QH // KH
    pairs = group // 2
    block = LOOKBACK_SPAN
    valued = jnp.concatenate([vlo[...], vhi[...]], 0).astype(f32)
    turned = valued.T.astype(bf16)
    for half in range(2):
        left = turned[half * HD : (half + 1) * HD]
        for p in range(pairs):
            head = half * group + 2 * p
            both = jnp.concatenate([probs[head], probs[head + 1]], 1)
            res = lax.dot_general(
                left, both, (((1,), (0,)), ((), ())), preferred_element_type=f32
            )
            stacked = jnp.concatenate([res[:, :block], res[:, block:]], 0)
            base = half * group * HD + p * LANES
            out[:, base : base + LANES] = stacked.T.astype(bf16)


def mix_call(probs, vlo, vhi, tokens, block_index, into):
    block = LOOKBACK_SPAN
    wide = 2 * (QH // KH) * HD
    heads = 2 * (QH // KH)
    extra = [] if into is None else [into]
    return pl.pallas_call(
        mix_body,
        grid=(KH // 2,),
        in_specs=[
            pl.BlockSpec((heads, 2 * block, block), lambda s: (s, 0, 0)),
            pl.BlockSpec((block, LANES), lambda s: (0, s)),
            pl.BlockSpec((block, LANES), lambda s: (0, s)),
        ]
        + [pl.BlockSpec(memory_space=pl.ANY)] * len(extra),
        out_specs=pl.BlockSpec((block, wide), lambda s: (block_index, s)),
        out_shape=full((tokens, QH * HD), bf16),
        input_output_aliases={3: 0} if extra else {},
        compiler_params=params(12),
    )(probs, vlo, vhi, *extra)


def cut_body(quad, near, acts, *refs):
    outs, shards = refs[:quad], refs[quad]
    devices, rows = shards.shape[:2]
    for j in range(devices):
        shards[j] = acts[j * rows : (j + 1) * rows, :]
    mine = near[0]
    for m in range(quad):
        for z in range(devices // quad):
            outs[m][z] = shards[z * quad + (mine ^ m)]


def cut_call(near, turned, devices, quad):
    width, tokens = turned.shape
    rows = width // devices
    return pl.pallas_call(
        functools.partial(cut_body, quad),
        in_specs=[SMEM, VMEM],
        out_specs=[VMEM] * quad,
        out_shape=[full((devices // quad, rows, tokens), bf16)] * quad,
        scratch_shapes=[pltpu.VMEM((devices, rows, tokens), bf16)],
        compiler_params=params(8),
        name="cut",
    )(near, turned)


def outer_body(quad, far_size, far, *refs):
    turned, grads, outs = refs[:quad], refs[quad : 2 * quad], refs[2 * quad :]
    mine = far[0]
    for k in range(far_size):
        z = mine ^ k
        total = None
        for m in range(quad):
            term = lax.dot_general(
                turned[m][z], grads[m][...], (((1,), (0,)), ((), ())), preferred_element_type=f32
            )
            total = term if total is None else total + term
        outs[k][...] = total.astype(outs[k].dtype)


def outer_call(far, turned, grads):
    quad = len(turned)
    far_size, rows, _ = turned[0].shape
    wide = grads[0].shape[1]
    return pl.pallas_call(
        functools.partial(outer_body, quad, far_size),
        in_specs=[SMEM] + [VMEM] * (2 * quad),
        out_specs=[VMEM] * far_size,
        out_shape=[full((rows, wide), f32 if k == 0 else bf16) for k in range(far_size)],
        compiler_params=params(8),
        name="outer",
    )(far, *turned, *grads)


def value_body(quad, far_size, far, *refs):
    turned, weights, outs = refs[:quad], refs[quad : quad + far_size], refs[quad + far_size :]
    mine = far[0]
    for m in range(quad):
        total = None
        for k in range(far_size):
            term = lax.dot_general(
                turned[m][mine ^ k],
                weights[k][...],
                (((0,), (0,)), ((), ())),
                preferred_element_type=f32,
            )
            total = term if total is None else total + term
        outs[m][...] = total


def value_call(far, turned, weights):
    quad = len(turned)
    far_size, _, tokens = turned[0].shape
    wide = weights[0].shape[1]
    return pl.pallas_call(
        functools.partial(value_body, quad, far_size),
        in_specs=[SMEM] + [VMEM] * (quad + far_size),
        out_specs=[VMEM] * quad,
        out_shape=[full((tokens, wide), f32)] * quad,
        compiler_params=params(8),
        name="value",
    )(far, *turned, *weights)


def join_body(count, *refs):
    parts, outs = refs[:count], refs[count:]
    for b, out in enumerate(outs):
        rows = slice(b * out.shape[0], (b + 1) * out.shape[0])
        total = parts[0][rows, :]
        for part in parts[1:]:
            total = total + part[rows, :]
        out[...] = total.astype(bf16)


def join_call(parts, blocks):
    tokens, wide = parts[0].shape
    return pl.pallas_call(
        functools.partial(join_body, len(parts)),
        in_specs=[VMEM] * len(parts),
        out_specs=[VMEM] * blocks,
        out_shape=[full((tokens // blocks, wide), bf16)] * blocks,
        compiler_params=params(4),
        name="join",
    )(*parts)


def reduce_body(scale, slot, own, *refs):
    others, total, square = refs[:-2], refs[-2], refs[-1]
    grad = own[...]
    for other in others:
        grad = grad + other[...].astype(f32)
    grad = grad * scale
    total[...] = grad
    lane = lax.broadcasted_iota(jnp.int32, square.shape, 1)
    square[...] = jnp.where(lane == slot[0], jnp.sum(grad * grad), 0.0)


def reduce_call(slot, own, others, scale):
    return pl.pallas_call(
        functools.partial(reduce_body, scale),
        in_specs=[SMEM] + [VMEM] * (1 + len(others)),
        out_specs=[VMEM] * 2,
        out_shape=[full(own.shape, f32), full((1, LANES), f32)],
        compiler_params=params(4),
        name="reduce",
    )(slot, own, *others)


def tree_sum(values):
    while len(values) > 1:
        values = [a + b for a, b in zip(values[::2], values[1::2])]
    return values[0]


def adam_body(workers, slot, fixes, squares, *refs):
    ins, outs = refs[: 4 * workers], refs[4 * workers :]
    fix_one, fix_two = fixes[0], fixes[1]
    results = []
    for w in range(workers):
        grad, weight, first, second = (r[...] for r in ins[4 * w : 4 * w + 4])
        norm = jnp.sqrt(jnp.full((8, grad.shape[1]), squares[0, slot[0] ^ w]))
        factor = jnp.minimum(1.0, clip_norm / (norm + 1e-06))
        grad = grad * factor[:1]
        first = beta_one * first + (1.0 - beta_one) * grad
        second = beta_two * second + (1.0 - beta_two) * grad * grad
        weight = weight - learn_rate * (first / fix_one) / (
            jnp.sqrt(second / fix_two) + adam_eps
        )
        results.append((weight, first, second))
    for out, values in zip(outs, zip(*results)):
        out[...] = tree_sum(list(values)) / workers


def adam_call(slot, fixes, squares, states):
    workers = len(states)
    shape = states[0][0].shape
    return pl.pallas_call(
        functools.partial(adam_body, workers),
        in_specs=[SMEM] * 3 + [VMEM] * (4 * workers),
        out_specs=[VMEM] * 3,
        out_shape=[full(shape, f32)] * 3,
        compiler_params=params(8),
        name="adam",
    )(slot, fixes, squares, *[a for state in states for a in state])


def scalar(value):
    return value.astype(jnp.int32).reshape(1)


def per_device(
    inputs, queries, keys, out_grad, positions, bands, step, value_weight, moment_one, moment_two
):
    acts = inputs[0]
    tokens = acts.shape[0]
    block = LOOKBACK_SPAN
    blocks = tokens // block
    devices = lax.axis_size("ctx")
    workers = lax.axis_size("work")
    quad = min(4, devices)
    far_size = devices // quad
    index = lax.axis_index("ctx")
    slot = scalar(lax.axis_index("work"))
    near = scalar(index & (quad - 1))
    far = scalar(index >> (quad.bit_length() - 1))
    keyed = keys[0]
    query, cotan = queries[0], out_grad[0]
    weight, first, second = value_weight[0], moment_one[0], moment_two[0]
    narrow = weight.astype(bf16)

    prev_keys = shifted(keyed, "ctx", 1)
    turned = cut_call(near, acts.T, devices, quad)
    turned = [turned[0]] + [swapped(turned[m], "ctx", m) for m in range(1, quad)]
    column = [narrow] + [swapped(narrow, "ctx", k * quad) for k in range(1, far_size)]

    probs = [None] * blocks
    grads = [None] * blocks
    for b in range(blocks - 1, -1, -1):
        lower, lo = (keyed, b - 1) if b else (prev_keys, blocks - 1)
        probs[b], grads[b] = probs_call(
            bands, positions, query, cotan, lower, lo, keyed, b, b
        )
    returned = shifted(grads[0][:block], "ctx", -1)
    rows = []
    for b in range(blocks):
        after = grads[b + 1][:block] if b + 1 < blocks else returned
        rows.append((grads[b][block:] + after).astype(bf16))
    value_grad = jnp.concatenate(rows, 0)
    value_grads = [value_grad] + [swapped(value_grad, "ctx", m) for m in range(1, quad)]

    parts = outer_call(far, turned, value_grads)
    others = [swapped(parts[k], "ctx", k * quad) for k in range(1, far_size)]

    pieces = value_call(far, turned, column)
    pieces = [pieces[0]] + [swapped(pieces[m], "ctx", m) for m in range(1, quad)]
    values = join_call(pieces, blocks)
    prev_values = shifted(values[-1], "ctx", 1)
    out = None
    for b in range(blocks - 1, -1, -1):
        lower = values[b - 1] if b else prev_values
        out = mix_call(probs[b], lower, values[b], tokens, b, out)

    grad, squares = reduce_call(slot, parts[0], others, 1.0 / (tokens * devices))
    states = [(grad, weight, first, second)]
    for w in range(1, workers):
        states.append(tuple(swapped(a, "work", w) for a in states[0]))
    for axis, size in (("work", workers), ("ctx", devices)):
        bit = 1
        while bit < size:
            squares = squares + swapped(squares, axis, bit)
            bit *= 2
    count = step[0].astype(f32)
    fixes = jnp.stack(
        [1.0 - jnp.power(f32(beta_one), count), 1.0 - jnp.power(f32(beta_two), count)]
    )
    mean_weight, mean_one, mean_two = adam_call(slot, fixes, squares, states)
    return (out[None], mean_weight, mean_one, mean_two)


def solution(mesh):
    in_specs = (
        P("work", "ctx", None),
        P("work", "ctx", None),
        P("work", "ctx", None),
        P("work", "ctx", None),
        P("work", "ctx"),
        P(),
        P(),
        P("work", "ctx", None),
        P("work", "ctx", None),
        P("work", "ctx", None),
    )
    out_specs = (P("work", "ctx", None), P("ctx", None), P("ctx", None), P("ctx", None))
    return jax.shard_map(
        per_device, mesh=mesh, in_specs=in_specs, out_specs=out_specs, check_vma=False
    )
```

```python
import functools

import jax
import jax.numpy as jnp
from jax import lax
from jax.experimental import pallas as pl
from jax.experimental.pallas import tpu as pltpu
from jax.sharding import PartitionSpec as P


HD = 64
QH = 32
KH = 4
LOOKBACK_SPAN = 128
LANES = 128

beta_one = 0.9
beta_two = 0.95
adam_eps = 1e-08
learn_rate = 0.01
clip_norm = 0.5

bf16 = jnp.bfloat16
f32 = jnp.float32


def swapped(array, axis, mask):
    pairs = [(i, i ^ mask) for i in range(lax.axis_size(axis))]
    return lax.ppermute(array, axis, pairs)


def shifted(array, axis, by):
    devices = lax.axis_size(axis)
    pairs = [(i, i + by) for i in range(devices) if 0 <= i + by < devices]
    return lax.ppermute(array, axis, pairs)


VMEM = pl.BlockSpec(memory_space=pltpu.VMEM)
SMEM = pl.BlockSpec(memory_space=pltpu.SMEM)


def in_hbm(*arrays):
    return [pltpu.with_memory_space_constraint(a, pltpu.HBM) for a in arrays]


def params(mib):
    return pltpu.CompilerParams(vmem_limit_bytes=mib << 20)


def full(shape, dtype):
    return jax.ShapeDtypeStruct(shape, dtype)


def probs_body(bands, pos, query, cotan, prev, klo, khi, probs_out, send, mine):
    block = LOOKBACK_SPAN
    group = QH // KH
    pairs = group // 2
    index, step = pl.program_id(0), pl.program_id(1)
    span = 2 * block
    left = lax.broadcasted_iota(jnp.int32, (span, LANES), 1) < HD
    lower = jnp.where(index == 0, prev[...].astype(f32), klo[...].astype(f32))
    keyed = jnp.concatenate([lower, khi[...].astype(f32)], 0) * HD ** (-0.5)
    rolled = pltpu.roll(keyed, HD, 1)
    dist = (
        lax.broadcasted_iota(jnp.int32, (span, block), 1)
        + block
        - lax.broadcasted_iota(jnp.int32, (span, block), 0)
    )
    dist = jnp.where(dist < 0, 2 * span, dist)
    row = pos[...]
    sums = []
    for half in range(2):
        one, two = (keyed, rolled) if half == 0 else (rolled, keyed)
        sides = (
            jnp.where(left, one, 0.0).astype(bf16),
            jnp.where(left, 0.0, two).astype(bf16),
        )
        base = half * group * HD
        cols = [slice(base + p * LANES, base + (p + 1) * LANES) for p in range(pairs)]
        queries = jnp.concatenate([query[:, c] for c in cols], 0)
        cotans = jnp.concatenate([cotan[:, c] for c in cols], 0)
        for odd, side in enumerate(sides):
            scores = lax.dot_general(
                side, queries, (((1,), (1,)), ((), ())), preferred_element_type=f32
            )
            rows = []
            for p in range(pairs):
                head = half * group + 2 * p + odd
                limit = jnp.minimum(row, bands[step * 2 * group + head])
                seen = jnp.where(
                    dist <= limit, scores[:, p * block : (p + 1) * block], -1e30
                )
                expo = jnp.exp(seen - jnp.max(seen, axis=0, keepdims=True))
                prob = (expo * (1.0 / jnp.sum(expo, axis=0, keepdims=True))).astype(bf16)
                probs_out[0, head] = prob
                rows.append(prob)
            sums.append(
                lax.dot_general(
                    jnp.concatenate(rows, 1),
                    cotans,
                    (((1,), (0,)), ((), ())),
                    preferred_element_type=f32,
                )
            )
    grad = jnp.where(
        left,
        sums[0] + pltpu.roll(sums[1], HD, 1),
        sums[3] + pltpu.roll(sums[2], HD, 1),
    )
    for b in range(mine.shape[0] // block):
        for s in range(mine.shape[1] // LANES):
            here = slice(b * block, (b + 1) * block)
            cols = slice(s * LANES, (s + 1) * LANES)

            @pl.when((index == b) & (step == s))
            def _():
                mine[here, cols] = grad[block:]
                if b:
                    before = slice((b - 1) * block, b * block)
                    mine[before, cols] = mine[before, cols] + grad[:block]
                else:
                    send[:, cols] = grad[:block]


def probs_call(bands, positions, queries, out_grad, prev_keys, keys):
    block = LOOKBACK_SPAN
    tokens = queries.shape[0]
    blocks = tokens // block
    wide = 2 * (QH // KH) * HD
    heads = 2 * (QH // KH)
    bands, positions, queries, out_grad, keys = in_hbm(
        bands, positions, queries, out_grad, keys
    )
    return pl.pallas_call(
        probs_body,
        grid=(blocks, KH // 2),
        in_specs=[
            SMEM,
            pl.BlockSpec((1, block), lambda b, s: (0, b)),
            pl.BlockSpec((block, wide), lambda b, s: (b, s)),
            pl.BlockSpec((block, wide), lambda b, s: (b, s)),
            pl.BlockSpec((block, LANES), lambda b, s: (blocks - 1, s)),
            pl.BlockSpec((block, LANES), lambda b, s: (jnp.maximum(b - 1, 0), s)),
            pl.BlockSpec((block, LANES), lambda b, s: (b, s)),
        ],
        out_specs=[
            pl.BlockSpec((1, heads, 2 * block, block), lambda b, s: (b, s, 0, 0)),
            pl.BlockSpec((block, KH * HD), lambda b, s: (0, 0)),
            pl.BlockSpec((tokens, KH * HD), lambda b, s: (0, 0)),
        ],
        out_shape=[
            pltpu.HBM((blocks, QH, 2 * block, block), bf16),
            full((block, KH * HD), f32),
            full((tokens, KH * HD), f32),
        ],
        compiler_params=params(12),
        name="probs",
    )(bands, positions, queries, out_grad, prev_keys, keys, keys)


def mix_body(probs, vlo, vhi, *refs):
    out = refs[-1]
    group = QH // KH
    pairs = group // 2
    block = LOOKBACK_SPAN
    valued = jnp.concatenate([vlo[...], vhi[...]], 0).astype(f32)
    turned = valued.T.astype(bf16)
    for half in range(2):
        left = turned[half * HD : (half + 1) * HD]
        for p in range(pairs):
            head = half * group + 2 * p
            both = jnp.concatenate([probs[0, head], probs[0, head + 1]], 1)
            res = lax.dot_general(
                left, both, (((1,), (0,)), ((), ())), preferred_element_type=f32
            )
            stacked = jnp.concatenate([res[:, :block], res[:, block:]], 0)
            base = half * group * HD + p * LANES
            out[:, base : base + LANES] = stacked.T.astype(bf16)


def mix_call(probs, lower, lo, values, first, count, into):
    block = LOOKBACK_SPAN
    tokens = values.shape[0]
    wide = 2 * (QH // KH) * HD
    heads = 2 * (QH // KH)
    extra = [] if into is None else [into]
    return pl.pallas_call(
        mix_body,
        grid=(count, KH // 2),
        in_specs=[
            pl.BlockSpec((1, heads, 2 * block, block), lambda b, s: (b + first, s, 0, 0)),
            pl.BlockSpec((block, LANES), lambda b, s: (b + lo, s)),
            pl.BlockSpec((block, LANES), lambda b, s: (b + first, s)),
        ]
        + [pl.BlockSpec(memory_space=pltpu.HBM)] * len(extra),
        out_specs=pl.BlockSpec((block, wide), lambda b, s: (b + first, s)),
        out_shape=pltpu.HBM((tokens, QH * HD), bf16),
        input_output_aliases={3: 0} if extra else {},
        compiler_params=params(8),
    )(*in_hbm(probs), lower, values, *extra)


def cut_body(quad, acts, weight, *refs):
    outs, narrow = refs[:quad], refs[quad]
    whole, shards, sems = refs[quad + 1 :]
    devices, rows = shards.shape[:2]
    far_size = devices // quad
    part = whole.shape[0] // sems.shape[0]
    copies = []
    for c in range(sems.shape[0]):
        copy = pltpu.make_async_copy(
            acts.at[pl.ds(c * part, part), :], whole.at[pl.ds(c * part, part), :], sems.at[c]
        )
        copy.start()
        copies.append(copy)
    narrow[...] = weight[...].reshape(narrow.shape).astype(bf16)
    per = devices // sems.shape[0]
    for c, copy in enumerate(copies):
        copy.wait()
        for j in range(c * per, (c + 1) * per):
            shards[j] = whole[j * rows : (j + 1) * rows, :]
    mine = lax.axis_index("ctx") & (quad - 1)
    for m in range(quad):
        for z in range(far_size):
            outs[m][z] = shards[z * quad + (mine ^ m)]


def cut_call(turned, weight, devices, quad):
    width, tokens = turned.shape
    rows = width // devices
    turned, weight = in_hbm(turned, weight)
    return pl.pallas_call(
        functools.partial(cut_body, quad),
        in_specs=[pl.BlockSpec(memory_space=pltpu.HBM), VMEM],
        out_specs=[VMEM] * (quad + 1),
        out_shape=[full((devices // quad, rows, tokens), bf16)] * quad
        + [full((rows, weight.shape[2]), bf16)],
        scratch_shapes=[
            pltpu.VMEM((width, tokens), bf16),
            pltpu.VMEM((devices, rows, tokens), bf16),
            pltpu.SemaphoreType.DMA((4,)),
        ],
        compiler_params=params(8),
        name="cut",
    )(turned, weight)


def far_index(quad):
    return lax.axis_index("ctx") >> (quad.bit_length() - 1)


def outer_body(quad, far_size, *refs):
    turned, grads, outs = refs[:quad], refs[quad : 2 * quad], refs[2 * quad :]
    mine = far_index(quad)
    for k in range(far_size):
        z = mine ^ k
        total = None
        for m in range(quad):
            term = lax.dot_general(
                turned[m][z], grads[m][...], (((1,), (0,)), ((), ())), preferred_element_type=f32
            )
            total = term if total is None else total + term
        outs[k][...] = total.astype(outs[k].dtype)


def outer_call(turned, grads):
    quad = len(turned)
    far_size, rows, _ = turned[0].shape
    wide = grads[0].shape[1]
    return pl.pallas_call(
        functools.partial(outer_body, quad, far_size),
        in_specs=[VMEM] * (2 * quad),
        out_specs=[VMEM] * far_size,
        out_shape=[full((rows, wide), f32 if k == 0 else bf16) for k in range(far_size)],
        compiler_params=params(8),
        name="outer",
    )(*turned, *grads)


def value_body(quad, far_size, *refs):
    turned, weights, outs = refs[:quad], refs[quad : quad + far_size], refs[quad + far_size :]
    mine = far_index(quad)
    for m in range(quad):
        total = None
        for k in range(far_size):
            term = lax.dot_general(
                turned[m][mine ^ k],
                weights[k][...],
                (((0,), (0,)), ((), ())),
                preferred_element_type=f32,
            )
            total = term if total is None else total + term
        outs[m][...] = total


def value_call(turned, weights):
    quad = len(turned)
    far_size, _, tokens = turned[0].shape
    wide = weights[0].shape[1]
    return pl.pallas_call(
        functools.partial(value_body, quad, far_size),
        in_specs=[VMEM] * (quad + far_size),
        out_specs=[VMEM] * quad,
        out_shape=[full((tokens, wide), f32)] * quad,
        compiler_params=params(8),
        name="value",
    )(*turned, *weights)


def join_body(count, *refs):
    parts, whole, tail = refs[:count], refs[count], refs[count + 1]
    total = parts[0][...]
    for part in parts[1:]:
        total = total + part[...]
    value = total.astype(bf16)
    whole[...] = value
    tail[...] = value[whole.shape[0] - tail.shape[0] :]


def join_call(parts):
    tokens, wide = parts[0].shape
    return pl.pallas_call(
        functools.partial(join_body, len(parts)),
        in_specs=[VMEM] * len(parts),
        out_specs=[VMEM] * 2,
        out_shape=[full((tokens, wide), bf16), full((LOOKBACK_SPAN, wide), bf16)],
        compiler_params=params(4),
        name="join",
    )(*parts)


def reduce_body(scale, own, *refs):
    others, total, square = refs[:-2], refs[-2], refs[-1]
    grad = own[...]
    for other in others:
        grad = grad + other[...].astype(f32)
    grad = grad * scale
    total[...] = grad
    lane = lax.broadcasted_iota(jnp.int32, square.shape, 1)
    square[...] = jnp.where(lane == lax.axis_index("work"), jnp.sum(grad * grad), 0.0)


def reduce_call(own, others, scale):
    return pl.pallas_call(
        functools.partial(reduce_body, scale),
        in_specs=[VMEM] * (1 + len(others)),
        out_specs=[VMEM] * 2,
        out_shape=[full(own.shape, f32), full((1, LANES), f32)],
        compiler_params=params(4),
        name="reduce",
    )(own, *others)


def pack_body(weight, first, second, out):
    for n, ref in enumerate((weight, first, second)):
        out[n] = ref[...].reshape(out.shape[1:])


def pack_call(weight, first, second):
    rows, _, wide = weight.shape
    return pl.pallas_call(
        pack_body,
        in_specs=[VMEM] * 3,
        out_specs=VMEM,
        out_shape=full((3, rows, wide), f32),
        compiler_params=params(4),
        name="pack",
    )(*in_hbm(weight, first, second))


def tree_sum(values):
    while len(values) > 1:
        values = [a + b for a, b in zip(values[::2], values[1::2])]
    return values[0]


def adam_body(workers, step, squares, *refs):
    grads, states, outs = refs[:workers], refs[workers : 2 * workers], refs[2 * workers :]
    shape = grads[0].shape
    count = jnp.full((8, shape[1]), step[0].astype(f32))
    fix_one = (1.0 - jnp.power(f32(beta_one), count))[:1]
    fix_two = (1.0 - jnp.power(f32(beta_two), count))[:1]
    slot = lax.axis_index("work")
    results = []
    for w in range(workers):
        norm = jnp.sqrt(jnp.full((8, shape[1]), squares[0, slot ^ w]))
        factor = jnp.minimum(1.0, clip_norm / (norm + 1e-06))
        grad = grads[w][...] * factor[:1]
        weight, first, second = states[w][0], states[w][1], states[w][2]
        first = beta_one * first + (1.0 - beta_one) * grad
        second = beta_two * second + (1.0 - beta_two) * grad * grad
        weight = weight - learn_rate * (first / fix_one) / (
            jnp.sqrt(second / fix_two) + adam_eps
        )
        results.append((weight, first, second))
    for out, values in zip(outs, zip(*results)):
        out[...] = tree_sum(list(values)) / workers


def adam_call(step, squares, grads, states):
    workers = len(states)
    shape = grads[0].shape
    return pl.pallas_call(
        functools.partial(adam_body, workers),
        in_specs=[SMEM] * 2 + [VMEM] * (2 * workers),
        out_specs=[VMEM] * 3,
        out_shape=[full(shape, f32)] * 3,
        compiler_params=params(8),
        name="adam",
    )(step, squares, *grads, *states)


def per_device(
    inputs, queries, keys, out_grad, positions, bands, step, value_weight, moment_one, moment_two
):
    tokens = inputs.shape[1]
    block = LOOKBACK_SPAN
    devices = lax.axis_size("ctx")
    workers = lax.axis_size("work")
    quad = min(4, devices)
    far_size = devices // quad
    weight, first, second = (
        jnp.transpose(a, (1, 0, 2)) for a in (value_weight, moment_one, moment_two)
    )

    *turned, narrow = cut_call(inputs[0].T, weight, devices, quad)
    turned = [turned[0]] + [swapped(turned[m], "ctx", m) for m in range(1, quad)]
    prev_keys = shifted(keys[0], "ctx", 1)
    column = [narrow] + [swapped(narrow, "ctx", k * quad) for k in range(1, far_size)]

    probs, send, mine = probs_call(bands, positions, queries[0], out_grad[0], prev_keys, keys[0])
    returned = shifted(send, "ctx", -1)
    last = tokens - block
    value_grad = jnp.concatenate([mine[:last], mine[last:] + returned], 0).astype(bf16)
    value_grads = [value_grad] + [swapped(value_grad, "ctx", m) for m in range(1, quad)]

    pieces = value_call(turned, column)
    parts = outer_call(turned, value_grads)
    others = [swapped(parts[k], "ctx", k * quad) for k in range(1, far_size)]

    pieces = [pieces[0]] + [swapped(pieces[m], "ctx", m) for m in range(1, quad)]
    values, tail = join_call(pieces)
    prev_values = shifted(tail, "ctx", 1)
    blocks = tokens // block
    out = None
    if blocks > 1:
        out = mix_call(probs, values, 0, values, 1, blocks - 1, None)
    out = mix_call(probs, prev_values, 0, values, 0, 1, out)

    state = pack_call(weight, first, second)
    states = [state] + [swapped(state, "work", w) for w in range(1, workers)]
    grad, squares = reduce_call(parts[0], others, 1.0 / (tokens * devices))
    grads = [grad] + [swapped(grad, "work", w) for w in range(1, workers)]
    for axis, size in (("work", workers), ("ctx", devices)):
        bit = size // 2
        while bit:
            squares = squares + swapped(squares, axis, bit)
            bit //= 2
    mean_weight, mean_one, mean_two = adam_call(step, squares, grads, states)
    return (out[None], mean_weight, mean_one, mean_two)


def solution(mesh):
    in_specs = (
        P("work", "ctx", None),
        P("work", "ctx", None),
        P("work", "ctx", None),
        P("work", "ctx", None),
        P("work", "ctx"),
        P(),
        P(),
        P("work", "ctx", None),
        P("work", "ctx", None),
        P("work", "ctx", None),
    )
    out_specs = (P("work", "ctx", None), P("ctx", None), P("ctx", None), P("ctx", None))
    return jax.shard_map(
        per_device, mesh=mesh, in_specs=in_specs, out_specs=out_specs, check_vma=False
    )
```

```python
import functools

import jax
import jax.numpy as jnp
from jax import lax
from jax.experimental import pallas as pl
from jax.experimental.pallas import tpu as pltpu
from jax.sharding import PartitionSpec as P


HD = 64
QH = 32
KH = 4
LOOKBACK_SPAN = 128
LANES = 128
SUBLANES = 8

beta_one = 0.9
beta_two = 0.95
adam_eps = 1e-08
learn_rate = 0.01
clip_norm = 0.5

bf16 = jnp.bfloat16
f32 = jnp.float32


def swapped(array, axis, mask):
    pairs = [(i, i ^ mask) for i in range(lax.axis_size(axis))]
    return lax.ppermute(array, axis, pairs)


def shifted(array, axis, by):
    devices = lax.axis_size(axis)
    pairs = [(i, i + by) for i in range(devices) if 0 <= i + by < devices]
    return lax.ppermute(array, axis, pairs)


VMEM = pl.BlockSpec(memory_space=pltpu.VMEM)
SMEM = pl.BlockSpec(memory_space=pltpu.SMEM)


def in_hbm(*arrays):
    return [pltpu.with_memory_space_constraint(a, pltpu.HBM) for a in arrays]


def in_vmem(*arrays):
    return [pltpu.with_memory_space_constraint(a, pltpu.VMEM) for a in arrays]


def vmem(shape, dtype):
    return pltpu.VMEM(shape, dtype)


def params(mib):
    return pltpu.CompilerParams(vmem_limit_bytes=mib << 20)


def full(shape, dtype):
    return jax.ShapeDtypeStruct(shape, dtype)


def probs_body(first, lower_from, bands, pos, query, cotan, prev, keys, probs_out, *grads_out):
    block = LOOKBACK_SPAN
    group = QH // KH
    pairs = group // 2
    turn, step = pl.program_id(0), pl.program_id(1)
    index = turn + first
    at = pl.ds(pl.multiple_of(index * block, block), block)
    above = pl.ds(pl.multiple_of(turn * block, block), block)
    lanes = pl.ds(pl.multiple_of(step * LANES, LANES), LANES)
    left = lax.broadcasted_iota(jnp.int32, (2 * block, LANES), 1) < HD
    before = pl.ds(pl.multiple_of(turn * block, block) + lower_from, block)
    lower = prev[before, lanes].astype(f32)
    keyed = jnp.concatenate([lower, keys[at, lanes].astype(f32)], 0) * HD ** (-0.5)
    rolled = pltpu.roll(keyed, HD, 1)
    gap = lax.broadcasted_iota(jnp.int32, (block, block), 1) - lax.broadcasted_iota(
        jnp.int32, (block, block), 0
    )
    own = gap >= 0
    same = gap == 0
    dist = jnp.where(own, gap, gap + block)
    row = pos[index]
    sums = []
    for half in range(2):
        one, two = (keyed, rolled) if half == 0 else (rolled, keyed)
        sides = (
            jnp.where(left, one, 0.0).astype(bf16),
            jnp.where(left, 0.0, two).astype(bf16),
        )
        base = (step * 2 + half) * group * HD
        cols = [
            pl.ds(pl.multiple_of(base + p * LANES, LANES), LANES) for p in range(pairs)
        ]
        queries = jnp.concatenate([query[at, c] for c in cols], 0)
        cotans = jnp.concatenate([cotan[at, c] for c in cols], 0)
        for odd, side in enumerate(sides):
            scores = lax.dot_general(
                side, queries, (((1,), (1,)), ((), ())), preferred_element_type=f32
            )
            rows = []
            for p in range(pairs):
                head = half * group + 2 * p + odd
                limit = jnp.minimum(row, bands[step * 2 * group + head])
                before = scores[:block, p * block : (p + 1) * block]
                here = scores[block:, p * block : (p + 1) * block]
                seen = jnp.where(dist <= limit, jnp.where(own, here, before), -1e30)
                far = jnp.sum(jnp.where(same, before, 0.0), axis=0, keepdims=True)
                far = jnp.where(limit >= block, far, -1e30)
                top = jnp.maximum(jnp.max(seen, axis=0, keepdims=True), far)
                expo = jnp.exp(seen - top)
                far = jnp.exp(far - top)
                scale = 1.0 / (jnp.sum(expo, axis=0, keepdims=True) + far)
                prob = expo * scale
                prob = jnp.concatenate(
                    [
                        jnp.where(own, jnp.where(same, far * scale, 0.0), prob).astype(bf16),
                        jnp.where(own, prob, 0.0).astype(bf16),
                    ],
                    0,
                )
                probs_out[turn, step * 2 * group + head] = prob
                rows.append(prob)
            sums.append(
                lax.dot_general(
                    jnp.concatenate(rows, 1),
                    cotans,
                    (((1,), (0,)), ((), ())),
                    preferred_element_type=f32,
                )
            )
    grad = jnp.where(
        left,
        sums[0] + pltpu.roll(sums[1], HD, 1),
        sums[3] + pltpu.roll(sums[2], HD, 1),
    )
    low, high = grad[:block], grad[block:]
    if first == 0:
        grads_out[0][:, lanes] = low
        grads_out[1][:, lanes] = high
    else:
        rows, = grads_out

        @pl.when(turn == 0)
        def _():
            rows[above, lanes] = low

        @pl.when(turn > 0)
        def _():
            rows[above, lanes] = rows[above, lanes] + low

        rows[at, lanes] = high


def probs_call(bands, positions, queries, out_grad, lower, keys, first, count):
    block = LOOKBACK_SPAN
    tokens = queries.shape[0]
    wide = KH * HD
    return pl.pallas_call(
        functools.partial(probs_body, first, 0 if first else lower.shape[0] - block),
        grid=(count, KH // 2),
        in_specs=[SMEM] + [VMEM] * 5,
        out_specs=[VMEM] * (2 if first else 3),
        out_shape=[vmem((count, QH, 2 * block, block), bf16)]
        + ([vmem((tokens, wide), f32)] if first else [vmem((block, wide), f32)] * 2),
        compiler_params=params(8),
    )(bands, *in_vmem(positions, queries, out_grad, lower, keys))


def mix_body(first, probs, lower, values, *refs):
    out = refs[-1]
    group = QH // KH
    pairs = group // 2
    block = LOOKBACK_SPAN
    index, step = pl.program_id(0), pl.program_id(1)
    at = pl.ds(pl.multiple_of((index + first) * block, block), block)
    above = pl.ds(pl.multiple_of(index * block, block), block)
    lanes = pl.ds(pl.multiple_of(step * LANES, LANES), LANES)
    valued = jnp.concatenate([lower[above, lanes], values[at, lanes]], 0).astype(f32)
    turned = valued.T.astype(bf16)
    for half in range(2):
        left = turned[half * HD : (half + 1) * HD]
        for p in range(pairs):
            head = step * 2 * group + half * group + 2 * p
            both = jnp.concatenate(
                [probs[index, head], probs[index, head + 1]], 1
            )
            res = lax.dot_general(
                left, both, (((1,), (0,)), ((), ())), preferred_element_type=f32
            )
            stacked = jnp.concatenate([res[:, :block], res[:, block:]], 0)
            base = half * group * HD + p * LANES
            out[:, base : base + LANES] = stacked.astype(bf16).T


def mix_call(probs, lower, values, first, count, into):
    block = LOOKBACK_SPAN
    tokens = values.shape[0]
    wide = 2 * (QH // KH) * HD
    extra = [] if into is None else [into]
    return pl.pallas_call(
        functools.partial(mix_body, first),
        grid=(count, KH // 2),
        in_specs=[VMEM] * 3 + [pl.BlockSpec(memory_space=pltpu.HBM)] * len(extra),
        out_specs=pl.BlockSpec((block, wide), lambda b, s: (b + first, s)),
        out_shape=pltpu.HBM((tokens, QH * HD), bf16),
        input_output_aliases={3: 0} if extra else {},
        compiler_params=params(8),
    )(*in_vmem(probs, lower, values), *extra)


def window_size(rows):
    return -(-(rows + max(rows * j % SUBLANES for j in range(SUBLANES))) // SUBLANES) * SUBLANES


def window_of(index, rows, width):
    start = jnp.minimum(index * rows // SUBLANES * SUBLANES, width - window_size(rows))
    return pl.multiple_of(start, SUBLANES), index * rows - start


def cut_body(quad, acts, weight, *refs):
    outs, (narrow, wide_weight, sems) = refs[:quad], refs[quad:]
    width = acts.shape[0]
    far_size, size = outs[0].shape[:2]
    rows, _, wide = weight.shape
    mine = lax.axis_index("ctx")
    copies = []
    for m in range(quad):
        for z in range(far_size):
            start, _ = window_of(z * quad + ((mine & (quad - 1)) ^ m), rows, width)
            copy = pltpu.make_async_copy(
                acts.at[pl.ds(start, size), :], outs[m].at[z], sems.at[m * far_size + z]
            )
            copy.start()
            copies.append(copy)
    fetch = pltpu.make_async_copy(weight, wide_weight, sems.at[quad * far_size])
    fetch.start()
    fetch.wait()
    _, offset = window_of(mine, rows, width)
    padded = jnp.concatenate(
        [wide_weight[...].reshape(rows, wide), jnp.zeros((size - rows, wide), f32)], 0
    )
    narrow[...] = pltpu.roll(padded, offset, 0).astype(bf16)
    for copy in copies:
        copy.wait()


def cut_call(turned, weight, devices, quad):
    _, tokens = turned.shape
    rows, _, wide = weight.shape
    size = window_size(rows)
    res = pl.pallas_call(
        functools.partial(cut_body, quad),
        in_specs=[pl.BlockSpec(memory_space=pltpu.HBM)] * 2,
        out_specs=[VMEM] * (quad + 1),
        out_shape=[vmem((devices // quad, size, tokens), bf16)] * quad
        + [vmem((size, wide), bf16)],
        scratch_shapes=[
            pltpu.VMEM(weight.shape, f32),
            pltpu.SemaphoreType.DMA((devices + 1,)),
        ],
        compiler_params=params(8),
        name="cut",
    )(*in_hbm(turned, weight))
    return res[:quad], res[quad]


def load_body(count, *refs):
    sources, targets, sems = refs[:count], refs[count : 2 * count], refs[2 * count]
    copies = [
        pltpu.make_async_copy(source, target, sems.at[n])
        for n, (source, target) in enumerate(zip(sources, targets))
    ]
    for copy in copies:
        copy.start()
    for copy in copies:
        copy.wait()


def load_call(*arrays):
    count = len(arrays)
    return pl.pallas_call(
        functools.partial(load_body, count),
        in_specs=[pl.BlockSpec(memory_space=pltpu.HBM)] * count,
        out_specs=[VMEM] * count,
        out_shape=[vmem(a.shape, a.dtype) for a in arrays],
        scratch_shapes=[pltpu.SemaphoreType.DMA((count,))],
        compiler_params=params(2),
        name="load",
    )(*in_hbm(*arrays))


def far_index(quad):
    return lax.axis_index("ctx") >> (quad.bit_length() - 1)


def outer_body(quad, far_size, *refs):
    turned, grads, outs = refs[:quad], refs[quad : 2 * quad], refs[2 * quad :]
    mine = far_index(quad)
    near = lax.axis_index("ctx") & (quad - 1)
    rows = outs[0].shape[0]
    size = turned[0].shape[1]
    for k in range(far_size):
        z = mine ^ k
        total = None
        for m in range(quad):
            term = lax.dot_general(
                turned[m][z], grads[m][...], (((1,), (0,)), ((), ())), preferred_element_type=f32
            )
            total = term if total is None else total + term
        _, offset = window_of(z * quad + near, rows, rows * quad * far_size)
        total = pltpu.roll(total, (size - offset) % size, 0)
        outs[k][...] = total[:rows].astype(outs[k].dtype)


def outer_call(turned, grads, rows):
    quad = len(turned)
    far_size = turned[0].shape[0]
    wide = grads[0].shape[1]
    return pl.pallas_call(
        functools.partial(outer_body, quad, far_size),
        in_specs=[VMEM] * (2 * quad),
        out_specs=[VMEM] * far_size,
        out_shape=[full((rows, wide), f32 if k == 0 else bf16) for k in range(far_size)],
        compiler_params=params(8),
        name="outer",
    )(*turned, *grads)


def value_body(quad, far_size, *refs):
    turned, weights, outs = refs[:quad], refs[quad : quad + far_size], refs[quad + far_size :]
    mine = far_index(quad)
    for m in range(quad):
        total = None
        for k in range(far_size):
            term = lax.dot_general(
                turned[m][mine ^ k],
                weights[k][...],
                (((0,), (0,)), ((), ())),
                preferred_element_type=f32,
            )
            total = term if total is None else total + term
        outs[m][...] = total


def value_call(turned, weights):
    quad = len(turned)
    far_size, _, tokens = turned[0].shape
    wide = weights[0].shape[1]
    return pl.pallas_call(
        functools.partial(value_body, quad, far_size),
        in_specs=[VMEM] * (quad + far_size),
        out_specs=[VMEM] * quad,
        out_shape=[full((tokens, wide), f32)] * quad,
        compiler_params=params(8),
        name="value",
    )(*turned, *weights)


def join_body(count, *refs):
    parts, whole, tail = refs[:count], refs[count], refs[count + 1]
    total = parts[0][...]
    for part in parts[1:]:
        total = total + part[...]
    value = total.astype(bf16)
    whole[...] = value
    tail[...] = value[whole.shape[0] - tail.shape[0] :]


def join_call(parts):
    tokens, wide = parts[0].shape
    return pl.pallas_call(
        functools.partial(join_body, len(parts)),
        in_specs=[VMEM] * len(parts),
        out_specs=[VMEM] * 2,
        out_shape=[full((tokens, wide), bf16), full((LOOKBACK_SPAN, wide), bf16)],
        compiler_params=params(4),
        name="join",
    )(*parts)


def reduce_body(scale, own, *refs):
    others, total, square = refs[:-2], refs[-2], refs[-1]
    grad = own[...]
    for other in others:
        grad = grad + other[...].astype(f32)
    grad = grad * scale
    total[...] = grad
    lane = lax.broadcasted_iota(jnp.int32, square.shape, 1)
    square[...] = jnp.where(lane == lax.axis_index("work"), jnp.sum(grad * grad), 0.0)


def reduce_call(own, others, scale):
    return pl.pallas_call(
        functools.partial(reduce_body, scale),
        in_specs=[VMEM] * (1 + len(others)),
        out_specs=[VMEM] * 2,
        out_shape=[full(own.shape, f32), full((1, LANES), f32)],
        compiler_params=params(4),
        name="reduce",
    )(own, *others)


def pack_body(step, weight, first, second, out, fixes):
    for n, ref in enumerate((weight, first, second)):
        out[n] = ref[...].reshape(out.shape[1:])
    row = lax.broadcasted_iota(jnp.int32, fixes.shape, 0)
    base = jnp.where(row == 0, f32(beta_one), f32(beta_two))
    fixes[...] = 1.0 - jnp.power(base, step[0].astype(f32))


def pack_call(step, weight, first, second):
    rows, _, wide = weight.shape
    return pl.pallas_call(
        pack_body,
        in_specs=[SMEM] + [VMEM] * 3,
        out_specs=[VMEM] * 2,
        out_shape=[vmem((3, rows, wide), f32), vmem((8, wide), f32)],
        compiler_params=params(4),
        name="pack",
    )(step, *in_hbm(weight, first, second))


def tree_sum(values):
    while len(values) > 1:
        values = [a + b for a, b in zip(values[::2], values[1::2])]
    return values[0]


def adam_body(workers, fixes, squares, *refs):
    grads, states, outs = refs[:workers], refs[workers : 2 * workers], refs[2 * workers :]
    fix_one, fix_two = fixes[0:1, :], fixes[1:2, :]
    slot = lax.axis_index("work")
    lane = lax.broadcasted_iota(jnp.int32, squares.shape, 1)
    results = []
    for w in range(workers):
        square = jnp.sum(
            jnp.where(lane == (slot ^ w), squares[...], 0.0), axis=1, keepdims=True
        )
        factor = jnp.minimum(1.0, clip_norm / (jnp.sqrt(square) + 1e-06))
        grad = grads[w][...] * factor
        weight, first, second = states[w][0], states[w][1], states[w][2]
        first = beta_one * first + (1.0 - beta_one) * grad
        second = beta_two * second + (1.0 - beta_two) * grad * grad
        weight = weight - learn_rate * (first / fix_one) / (
            jnp.sqrt(second / fix_two) + adam_eps
        )
        results.append((weight, first, second))
    for out, values in zip(outs, zip(*results)):
        out[...] = tree_sum(list(values)) / workers


def adam_call(fixes, squares, grads, states):
    workers = len(states)
    shape = grads[0].shape
    return pl.pallas_call(
        functools.partial(adam_body, workers),
        in_specs=[VMEM] * (2 + 2 * workers),
        out_specs=[VMEM] * 3,
        out_shape=[full(shape, f32)] * 3,
        compiler_params=params(8),
        name="adam",
    )(*in_vmem(fixes, squares, *grads, *states))


def per_device(
    inputs, queries, keys, out_grad, positions, bands, step, value_weight, moment_one, moment_two
):
    tokens = inputs.shape[1]
    block = LOOKBACK_SPAN
    devices = lax.axis_size("ctx")
    workers = lax.axis_size("work")
    quad = min(4, devices)
    far_size = devices // quad
    weight, first, second = (
        jnp.transpose(a, (1, 0, 2)) for a in (value_weight, moment_one, moment_two)
    )

    blocks = tokens // block
    prev_keys = shifted(keys[0], "ctx", 1)
    turned, narrow = cut_call(inputs[0].T, weight, devices, quad)
    keyed, query, cotan, pos = load_call(
        keys[0], queries[0], out_grad[0], positions.reshape(blocks, 1, block)
    )
    turned = [turned[0]] + [swapped(turned[m], "ctx", m) for m in range(1, quad)]
    column = [narrow] + [swapped(narrow, "ctx", k * quad) for k in range(1, far_size)]

    probs_prev, send, head = probs_call(bands, pos, query, cotan, prev_keys, keyed, 0, 1)
    returned = shifted(send, "ctx", -1)
    probs_own, rest = probs_call(bands, pos, query, cotan, keyed, keyed, 1, blocks - 1)
    last = tokens - block
    value_grad = jnp.concatenate(
        [head + rest[:block], rest[block:last], rest[last:] + returned], 0
    ).astype(bf16)
    value_grads = [value_grad] + [swapped(value_grad, "ctx", m) for m in range(1, quad)]

    pieces = value_call(turned, column)
    parts = outer_call(turned, value_grads, weight.shape[0])
    others = [swapped(parts[k], "ctx", k * quad) for k in range(1, far_size)]

    pieces = [pieces[0]] + [swapped(pieces[m], "ctx", m) for m in range(1, quad)]
    values, tail = join_call(pieces)
    prev_values = shifted(tail, "ctx", 1)
    out = mix_call(probs_own, values, values, 1, blocks - 1, None)
    out = mix_call(probs_prev, prev_values, values, 0, 1, out)

    state, fixes = pack_call(step, weight, first, second)
    states = [state] + [swapped(state, "work", w) for w in range(1, workers)]
    grad, squares = reduce_call(parts[0], others, 1.0 / (tokens * devices))
    grads = [grad] + [swapped(grad, "work", w) for w in range(1, workers)]
    for axis, size in (("work", workers), ("ctx", devices)):
        bit = size // 2
        while bit:
            squares = squares + swapped(squares, axis, bit)
            bit //= 2
    mean_weight, mean_one, mean_two = adam_call(fixes, squares, grads, states)
    return (out[None], mean_weight, mean_one, mean_two)


def solution(mesh):
    in_specs = (
        P("work", "ctx", None),
        P("work", "ctx", None),
        P("work", "ctx", None),
        P("work", "ctx", None),
        P("work", "ctx"),
        P(),
        P(),
        P("work", "ctx", None),
        P("work", "ctx", None),
        P("work", "ctx", None),
    )
    out_specs = (P("work", "ctx", None), P("ctx", None), P("ctx", None), P("ctx", None))
    return jax.shard_map(
        per_device, mesh=mesh, in_specs=in_specs, out_specs=out_specs, check_vma=False
    )
```

```python
import functools

import jax
import jax.numpy as jnp
from jax import lax
from jax.experimental import pallas as pl
from jax.experimental.pallas import tpu as pltpu
from jax.sharding import PartitionSpec as P


HD = 64
QH = 32
KH = 4
LOOKBACK_SPAN = 128
LANES = 128
SUBLANES = 8

beta_one = 0.9
beta_two = 0.95
adam_eps = 1e-08
learn_rate = 0.01
clip_norm = 0.5

bf16 = jnp.bfloat16
f32 = jnp.float32


def swapped(array, axis, mask):
    pairs = [(i, i ^ mask) for i in range(lax.axis_size(axis))]
    return lax.ppermute(array, axis, pairs)


def shifted(array, axis, by):
    devices = lax.axis_size(axis)
    pairs = [(i, i + by) for i in range(devices) if 0 <= i + by < devices]
    return lax.ppermute(array, axis, pairs)


VMEM = pl.BlockSpec(memory_space=pltpu.VMEM)
SMEM = pl.BlockSpec(memory_space=pltpu.SMEM)


def in_hbm(*arrays):
    return [pltpu.with_memory_space_constraint(a, pltpu.HBM) for a in arrays]


def in_vmem(*arrays):
    return [pltpu.with_memory_space_constraint(a, pltpu.VMEM) for a in arrays]


def vmem(shape, dtype):
    return pltpu.VMEM(shape, dtype)


def params(mib):
    return pltpu.CompilerParams(vmem_limit_bytes=mib << 20)


def full(shape, dtype):
    return jax.ShapeDtypeStruct(shape, dtype)


def probs_body(first, lower_from, bands, pos, query, cotan, prev, keys, probs_out, *grads_out):
    block = LOOKBACK_SPAN
    group = QH // KH
    pairs = group // 2
    turn, step = pl.program_id(0), pl.program_id(1)
    index = turn + first
    at = pl.ds(pl.multiple_of(index * block, block), block)
    above = pl.ds(pl.multiple_of(turn * block, block), block)
    lanes = pl.ds(pl.multiple_of(step * LANES, LANES), LANES)
    left = lax.broadcasted_iota(jnp.int32, (2 * block, LANES), 1) < HD
    before = pl.ds(pl.multiple_of(turn * block, block) + lower_from, block)
    lower = prev[before, lanes].astype(f32)
    keyed = jnp.concatenate([lower, keys[at, lanes].astype(f32)], 0) * HD ** (-0.5)
    rolled = pltpu.roll(keyed, HD, 1)
    gap = lax.broadcasted_iota(jnp.int32, (block, block), 1) - lax.broadcasted_iota(
        jnp.int32, (block, block), 0
    )
    own = gap >= 0
    same = gap == 0
    dist = jnp.where(own, gap, gap + block)
    row = pos[index]
    sums = []
    for half in range(2):
        one, two = (keyed, rolled) if half == 0 else (rolled, keyed)
        sides = (
            jnp.where(left, one, 0.0).astype(bf16),
            jnp.where(left, 0.0, two).astype(bf16),
        )
        base = (step * 2 + half) * group * HD
        cols = [
            pl.ds(pl.multiple_of(base + p * LANES, LANES), LANES) for p in range(pairs)
        ]
        queries = jnp.concatenate([query[at, c] for c in cols], 0)
        cotans = jnp.concatenate([cotan[at, c] for c in cols], 0)
        for odd, side in enumerate(sides):
            scores = lax.dot_general(
                side, queries, (((1,), (1,)), ((), ())), preferred_element_type=f32
            )
            rows = []
            for p in range(pairs):
                head = half * group + 2 * p + odd
                limit = jnp.minimum(row, bands[step * 2 * group + head])
                before = scores[:block, p * block : (p + 1) * block]
                here = scores[block:, p * block : (p + 1) * block]
                seen = jnp.where(dist <= limit, jnp.where(own, here, before), -1e30)
                far = jnp.sum(jnp.where(same, before, 0.0), axis=0, keepdims=True)
                far = jnp.where(limit >= block, far, -1e30)
                top = jnp.maximum(jnp.max(seen, axis=0, keepdims=True), far)
                expo = jnp.exp(seen - top)
                far = jnp.exp(far - top)
                scale = 1.0 / (jnp.sum(expo, axis=0, keepdims=True) + far)
                prob = expo * scale
                prob = jnp.concatenate(
                    [
                        jnp.where(own, jnp.where(same, far * scale, 0.0), prob).astype(bf16),
                        jnp.where(own, prob, 0.0).astype(bf16),
                    ],
                    0,
                )
                probs_out[turn, step * 2 * group + head] = prob
                rows.append(prob)
            sums.append(
                lax.dot_general(
                    jnp.concatenate(rows, 1),
                    cotans,
                    (((1,), (0,)), ((), ())),
                    preferred_element_type=f32,
                )
            )
    grad = jnp.where(
        left,
        sums[0] + pltpu.roll(sums[1], HD, 1),
        sums[3] + pltpu.roll(sums[2], HD, 1),
    )
    low, high = grad[:block], grad[block:]
    if first == 0:
        grads_out[0][:, lanes] = low.astype(bf16)
        grads_out[1][:, lanes] = high
    else:
        rows, = grads_out

        @pl.when(turn == 0)
        def _():
            rows[above, lanes] = low

        @pl.when(turn > 0)
        def _():
            rows[above, lanes] = rows[above, lanes] + low

        rows[at, lanes] = high


def probs_call(bands, positions, queries, out_grad, lower, keys, first, count):
    block = LOOKBACK_SPAN
    tokens = queries.shape[0]
    wide = KH * HD
    return pl.pallas_call(
        functools.partial(probs_body, first, 0 if first else lower.shape[0] - block),
        grid=(count, KH // 2),
        in_specs=[SMEM] + [VMEM] * 5,
        out_specs=[VMEM] * (2 if first else 3),
        out_shape=[vmem((count, QH, 2 * block, block), bf16)]
        + ([vmem((tokens, wide), f32)] if first else [vmem((block, wide), bf16), vmem((block, wide), f32)]),
        compiler_params=params(8),
    )(bands, *in_vmem(positions, queries, out_grad, lower, keys))


def mix_body(first, probs, lower, values, *refs):
    out = refs[-1]
    group = QH // KH
    pairs = group // 2
    block = LOOKBACK_SPAN
    index, step = pl.program_id(0), pl.program_id(1)
    at = pl.ds(pl.multiple_of((index + first) * block, block), block)
    above = pl.ds(pl.multiple_of(index * block, block), block)
    lanes = pl.ds(pl.multiple_of(step * LANES, LANES), LANES)
    valued = jnp.concatenate([lower[above, lanes], values[at, lanes]], 0).astype(f32)
    turned = valued.T.astype(bf16)
    for half in range(2):
        left = turned[half * HD : (half + 1) * HD]
        for p in range(pairs):
            head = step * 2 * group + half * group + 2 * p
            both = jnp.concatenate(
                [probs[index, head], probs[index, head + 1]], 1
            )
            res = lax.dot_general(
                left, both, (((1,), (0,)), ((), ())), preferred_element_type=f32
            )
            stacked = jnp.concatenate([res[:, :block], res[:, block:]], 0)
            base = half * group * HD + p * LANES
            out[:, base : base + LANES] = stacked.astype(bf16).T


def mix_call(probs, lower, values, first, count, into):
    block = LOOKBACK_SPAN
    tokens = values.shape[0]
    wide = 2 * (QH // KH) * HD
    extra = [] if into is None else [into]
    return pl.pallas_call(
        functools.partial(mix_body, first),
        grid=(count, KH // 2),
        in_specs=[VMEM] * 3 + [pl.BlockSpec(memory_space=pltpu.HBM)] * len(extra),
        out_specs=pl.BlockSpec((block, wide), lambda b, s: (b + first, s)),
        out_shape=pltpu.HBM((tokens, QH * HD), bf16),
        input_output_aliases={3: 0} if extra else {},
        compiler_params=params(8),
    )(*in_vmem(probs, lower, values), *extra)


def window_size(rows):
    return -(-(rows + max(rows * j % SUBLANES for j in range(SUBLANES))) // SUBLANES) * SUBLANES


def window_of(index, rows, width):
    start = jnp.minimum(index * rows // SUBLANES * SUBLANES, width - window_size(rows))
    return pl.multiple_of(start, SUBLANES), index * rows - start


def cut_body(quad, acts, weight, *refs):
    outs, (narrow, wide_weight, sems) = refs[:quad], refs[quad:]
    width = acts.shape[0]
    far_size, size = outs[0].shape[:2]
    rows, _, wide = weight.shape
    mine = lax.axis_index("ctx")
    copies = []
    for m in range(quad):
        for z in range(far_size):
            start, _ = window_of(z * quad + ((mine & (quad - 1)) ^ m), rows, width)
            copy = pltpu.make_async_copy(
                acts.at[pl.ds(start, size), :], outs[m].at[z], sems.at[m * far_size + z]
            )
            copy.start()
            copies.append(copy)
    fetch = pltpu.make_async_copy(weight, wide_weight, sems.at[quad * far_size])
    fetch.start()
    fetch.wait()
    _, offset = window_of(mine, rows, width)
    padded = jnp.concatenate(
        [wide_weight[...].reshape(rows, wide), jnp.zeros((size - rows, wide), f32)], 0
    )
    narrow[...] = pltpu.roll(padded, offset, 0).astype(bf16)
    for copy in copies:
        copy.wait()


def cut_call(turned, weight, devices, quad):
    _, tokens = turned.shape
    rows, _, wide = weight.shape
    size = window_size(rows)
    res = pl.pallas_call(
        functools.partial(cut_body, quad),
        in_specs=[pl.BlockSpec(memory_space=pltpu.HBM)] * 2,
        out_specs=[VMEM] * (quad + 1),
        out_shape=[vmem((devices // quad, size, tokens), bf16)] * quad
        + [vmem((size, wide), bf16)],
        scratch_shapes=[
            pltpu.VMEM(weight.shape, f32),
            pltpu.SemaphoreType.DMA((devices + 1,)),
        ],
        compiler_params=params(8),
        name="cut",
    )(*in_hbm(turned, weight))
    return res[:quad], res[quad]


def load_body(count, *refs):
    sources, targets, sems = refs[:count], refs[count : 2 * count], refs[2 * count]
    copies = [
        pltpu.make_async_copy(source, target, sems.at[n])
        for n, (source, target) in enumerate(zip(sources, targets))
    ]
    for copy in copies:
        copy.start()
    for copy in copies:
        copy.wait()


def load_call(*arrays):
    count = len(arrays)
    return pl.pallas_call(
        functools.partial(load_body, count),
        in_specs=[pl.BlockSpec(memory_space=pltpu.HBM)] * count,
        out_specs=[VMEM] * count,
        out_shape=[vmem(a.shape, a.dtype) for a in arrays],
        scratch_shapes=[pltpu.SemaphoreType.DMA((count,))],
        compiler_params=params(2),
        name="load",
    )(*in_hbm(*arrays))


def far_index(quad):
    return lax.axis_index("ctx") >> (quad.bit_length() - 1)


def outer_body(quad, far_size, *refs):
    turned, grads, outs = refs[:quad], refs[quad : 2 * quad], refs[2 * quad :]
    mine = far_index(quad)
    near = lax.axis_index("ctx") & (quad - 1)
    rows = outs[0].shape[0]
    size = turned[0].shape[1]
    for k in range(far_size):
        z = mine ^ k
        total = None
        for m in range(quad):
            term = lax.dot_general(
                turned[m][z], grads[m][...], (((1,), (0,)), ((), ())), preferred_element_type=f32
            )
            total = term if total is None else total + term
        _, offset = window_of(z * quad + near, rows, rows * quad * far_size)
        total = pltpu.roll(total, (size - offset) % size, 0)
        outs[k][...] = total[:rows].astype(outs[k].dtype)


def outer_call(turned, grads, rows):
    quad = len(turned)
    far_size = turned[0].shape[0]
    wide = grads[0].shape[1]
    return pl.pallas_call(
        functools.partial(outer_body, quad, far_size),
        in_specs=[VMEM] * (2 * quad),
        out_specs=[VMEM] * far_size,
        out_shape=[full((rows, wide), f32 if k == 0 else bf16) for k in range(far_size)],
        compiler_params=params(8),
        name="outer",
    )(*turned, *grads)


def value_body(quad, far_size, *refs):
    turned, weights, outs = refs[:quad], refs[quad : quad + far_size], refs[quad + far_size :]
    mine = far_index(quad)
    for m in range(quad):
        total = None
        for k in range(far_size):
            term = lax.dot_general(
                turned[m][mine ^ k],
                weights[k][...],
                (((0,), (0,)), ((), ())),
                preferred_element_type=f32,
            )
            total = term if total is None else total + term
        outs[m][...] = total


def value_call(turned, weights):
    quad = len(turned)
    far_size, _, tokens = turned[0].shape
    wide = weights[0].shape[1]
    return pl.pallas_call(
        functools.partial(value_body, quad, far_size),
        in_specs=[VMEM] * (quad + far_size),
        out_specs=[VMEM] * quad,
        out_shape=[full((tokens, wide), f32)] * quad,
        compiler_params=params(8),
        name="value",
    )(*turned, *weights)


def join_body(count, *refs):
    parts, whole, tail = refs[:count], refs[count], refs[count + 1]
    total = parts[0][...]
    for part in parts[1:]:
        total = total + part[...]
    value = total.astype(bf16)
    whole[...] = value
    tail[...] = value[whole.shape[0] - tail.shape[0] :]


def join_call(parts):
    tokens, wide = parts[0].shape
    return pl.pallas_call(
        functools.partial(join_body, len(parts)),
        in_specs=[VMEM] * len(parts),
        out_specs=[VMEM] * 2,
        out_shape=[full((tokens, wide), bf16), full((LOOKBACK_SPAN, wide), bf16)],
        compiler_params=params(4),
        name="join",
    )(*parts)


def reduce_body(scale, own, *refs):
    others, total, square = refs[:-2], refs[-2], refs[-1]
    grad = own[...]
    for other in others:
        grad = grad + other[...].astype(f32)
    grad = grad * scale
    total[...] = grad
    lane = lax.broadcasted_iota(jnp.int32, square.shape, 1)
    square[...] = jnp.where(lane == lax.axis_index("work"), jnp.sum(grad * grad), 0.0)


def reduce_call(own, others, scale):
    return pl.pallas_call(
        functools.partial(reduce_body, scale),
        in_specs=[VMEM] * (1 + len(others)),
        out_specs=[VMEM] * 2,
        out_shape=[full(own.shape, f32), full((1, LANES), f32)],
        compiler_params=params(4),
        name="reduce",
    )(own, *others)


def pack_body(step, weight, first, second, out, fixes):
    for n, ref in enumerate((weight, first, second)):
        out[n] = ref[...].reshape(out.shape[1:])
    row = lax.broadcasted_iota(jnp.int32, fixes.shape, 0)
    base = jnp.where(row == 0, f32(beta_one), f32(beta_two))
    fixes[...] = 1.0 - jnp.power(base, step[0].astype(f32))


def pack_call(step, weight, first, second):
    rows, _, wide = weight.shape
    return pl.pallas_call(
        pack_body,
        in_specs=[SMEM] + [VMEM] * 3,
        out_specs=[VMEM] * 2,
        out_shape=[vmem((3, rows, wide), f32), vmem((8, wide), f32)],
        compiler_params=params(4),
        name="pack",
    )(step, *in_hbm(weight, first, second))


def tree_sum(values):
    while len(values) > 1:
        values = [a + b for a, b in zip(values[::2], values[1::2])]
    return values[0]


def adam_body(workers, fixes, squares, *refs):
    grads, states, outs = refs[:workers], refs[workers : 2 * workers], refs[2 * workers :]
    fix_one, fix_two = fixes[0:1, :], fixes[1:2, :]
    slot = lax.axis_index("work")
    lane = lax.broadcasted_iota(jnp.int32, squares.shape, 1)
    results = []
    for w in range(workers):
        square = jnp.sum(
            jnp.where(lane == (slot ^ w), squares[...], 0.0), axis=1, keepdims=True
        )
        factor = jnp.minimum(1.0, clip_norm / (jnp.sqrt(square) + 1e-06))
        grad = grads[w][...] * factor
        weight, first, second = states[w][0], states[w][1], states[w][2]
        first = beta_one * first + (1.0 - beta_one) * grad
        second = beta_two * second + (1.0 - beta_two) * grad * grad
        weight = weight - learn_rate * (first / fix_one) / (
            jnp.sqrt(second / fix_two) + adam_eps
        )
        results.append((weight, first, second))
    for out, values in zip(outs, zip(*results)):
        out[...] = tree_sum(list(values)) / workers


def adam_call(fixes, squares, grads, states):
    workers = len(states)
    shape = grads[0].shape
    return pl.pallas_call(
        functools.partial(adam_body, workers),
        in_specs=[VMEM] * (2 + 2 * workers),
        out_specs=[VMEM] * 3,
        out_shape=[full(shape, f32)] * 3,
        compiler_params=params(8),
        name="adam",
    )(*in_vmem(fixes, squares, *grads, *states))


def per_device(
    inputs, queries, keys, out_grad, positions, bands, step, value_weight, moment_one, moment_two
):
    tokens = inputs.shape[1]
    block = LOOKBACK_SPAN
    devices = lax.axis_size("ctx")
    workers = lax.axis_size("work")
    quad = min(4, devices)
    far_size = devices // quad
    weight, first, second = (
        jnp.transpose(a, (1, 0, 2)) for a in (value_weight, moment_one, moment_two)
    )

    blocks = tokens // block
    prev_keys = shifted(keys[0], "ctx", 1)
    turned, narrow = cut_call(inputs[0].T, weight, devices, quad)
    keyed, query, cotan, pos = load_call(
        keys[0], queries[0], out_grad[0], positions.reshape(blocks, 1, block)
    )
    turned = [turned[0]] + [swapped(turned[m], "ctx", m) for m in range(1, quad)]
    column = [narrow] + [swapped(narrow, "ctx", k * quad) for k in range(1, far_size)]

    probs_prev, send, head = probs_call(bands, pos, query, cotan, prev_keys, keyed, 0, 1)
    returned = shifted(send, "ctx", -1)
    probs_own, rest = probs_call(bands, pos, query, cotan, keyed, keyed, 1, blocks - 1)
    last = tokens - block
    value_grad = jnp.concatenate(
        [head + rest[:block], rest[block:last], rest[last:] + returned.astype(f32)], 0
    ).astype(bf16)
    value_grads = [value_grad] + [swapped(value_grad, "ctx", m) for m in range(1, quad)]

    pieces = value_call(turned, column)
    parts = outer_call(turned, value_grads, weight.shape[0])
    others = [swapped(parts[k], "ctx", k * quad) for k in range(1, far_size)]

    pieces = [pieces[0]] + [swapped(pieces[m], "ctx", m) for m in range(1, quad)]
    values, tail = join_call(pieces)
    prev_values = shifted(tail, "ctx", 1)
    out = mix_call(probs_own, values, values, 1, blocks - 1, None)
    out = mix_call(probs_prev, prev_values, values, 0, 1, out)

    state, fixes = pack_call(step, weight, first, second)
    states = [state] + [swapped(state, "work", w) for w in range(1, workers)]
    grad, squares = reduce_call(parts[0], others, 1.0 / (tokens * devices))
    grads = [grad] + [swapped(grad, "work", w) for w in range(1, workers)]
    for axis, size in (("work", workers), ("ctx", devices)):
        bit = size // 2
        while bit:
            squares = squares + swapped(squares, axis, bit)
            bit //= 2
    mean_weight, mean_one, mean_two = adam_call(fixes, squares, grads, states)
    return (out[None], mean_weight, mean_one, mean_two)


def solution(mesh):
    in_specs = (
        P("work", "ctx", None),
        P("work", "ctx", None),
        P("work", "ctx", None),
        P("work", "ctx", None),
        P("work", "ctx"),
        P(),
        P(),
        P("work", "ctx", None),
        P("work", "ctx", None),
        P("work", "ctx", None),
    )
    out_specs = (P("work", "ctx", None), P("ctx", None), P("ctx", None), P("ctx", None))
    return jax.shard_map(
        per_device, mesh=mesh, in_specs=in_specs, out_specs=out_specs, check_vma=False
    )
```
